256 devices in a mesh: rows: 64 (over z_lo, x, y, core), rep: 4 (over z_hi).
Axes of the slice: x: 4, y: 4, z: 8 (z_hi: 4, z_lo: 2; z = z_hi * 2 + z_lo), core: 2. Of those that a mesh axis runs over, the one named last changes fastest.
Arguments:
- maps: float32 [4, 4096, 4096], P('rep', 'rows'), may hold values from -12 to 12
- mask: int32 [4096, 4096], P('rows'), may hold values 0 or 1
- bins: int32 [4096, 4096], P(None, 'rows'), may hold values from 0 to 1023
Outputs:
- spectra: float32 [2, 3, 1024], replicated
The draws below stay inside these ranges and needn't reach their ends.
All inputs are finite; a program needn't handle non-finite values. No bound on the sum of `mask` on one device may be relied on, other than what follows from the above.
Results may differ from the reference program's by a relative error of at most 0.0016.
Values sent between devices are 32-bit elements; how exact they have to be, the bound alone decides.
A program may use at most 64 MiB of HBM per device.

```python
import math
import jax
import jax.numpy as jnp
from jax import lax

SIDE = 4096
NBINS = 1024
SIMS = 2


def draw_bins(key, part):
    indices = lax.iota(jnp.int32, SIDE)
    signed = jnp.where(indices >= SIDE // 2, indices - SIDE, indices)
    squared = signed[:, None] * signed[:, None] + signed[None, :] * signed[None, :]
    radial = jnp.zeros_like(squared)
    for shift_bits in range(14, -1, -1):
        candidate = radial + (1 << shift_bits)
        radial = jnp.where(candidate * candidate <= squared, candidate, radial)
    offsets = jax.random.randint(jax.random.fold_in(key, 11), (SIDE, SIDE), -1, 2, dtype=jnp.int32)
    radius_cap = SIDE * 181 // 256 + 1
    return jnp.clip((radial + offsets) * NBINS // radius_cap, 0, NBINS - 1).astype(jnp.int32)


def sky_pair(key):
    mode_count = 16
    reach = max(24 * SIDE // NBINS, 4)
    keys = jax.random.split(key, 5)
    total = 2 * mode_count
    wave_y = jax.random.randint(keys[0], (total,), -reach, reach + 1, dtype=jnp.int32)
    wave_x = jax.random.randint(keys[1], (total,), -reach, reach + 1, dtype=jnp.int32)
    wave_x = jnp.where((wave_x == 0) & (wave_y == 0), 1, wave_x)
    strength = 1.5 / math.sqrt(NBINS) * jnp.exp(jax.random.uniform(keys[2], (total,), jnp.float32, -0.7, 0.7))
    phases = jax.random.uniform(keys[3], (total,), jnp.float32, -math.pi, math.pi)
    leakage = jax.random.uniform(keys[4], (total,), jnp.float32, -1.0, 1.0) * (math.sqrt(NBINS) / SIDE)
    float_y = wave_y.astype(jnp.float32)
    float_x = wave_x.astype(jnp.float32)
    squared = float_x * float_x + float_y * float_y
    cos_twice = (float_x * float_x - float_y * float_y) / squared
    sin_twice = 2.0 * float_x * float_y / squared
    is_curl = lax.iota(jnp.int32, total) >= mode_count
    q_amp = jnp.where(is_curl, -sin_twice, cos_twice - leakage * sin_twice) * strength
    u_amp = jnp.where(is_curl, cos_twice, sin_twice + leakage * cos_twice) * strength
    cells = lax.iota(jnp.int32, SIDE)
    along_y = jnp.mod(cells[:, None] * wave_y[None, :], SIDE).astype(jnp.float32) * (2.0 * math.pi / SIDE) + phases[None, :]
    along_x = jnp.mod(wave_x[:, None] * cells[None, :], SIDE).astype(jnp.float32) * (2.0 * math.pi / SIDE)
    right_factor = jnp.concatenate([jnp.cos(along_x), -jnp.sin(along_x)], axis=0)
    left_q = jnp.concatenate([jnp.cos(along_y) * q_amp[None, :], jnp.sin(along_y) * q_amp[None, :]], axis=1)
    left_u = jnp.concatenate([jnp.cos(along_y) * u_amp[None, :], jnp.sin(along_y) * u_amp[None, :]], axis=1)
    field_q = jnp.dot(left_q, right_factor, precision=lax.Precision.HIGHEST)
    field_u = jnp.dot(left_u, right_factor, precision=lax.Precision.HIGHEST)
    return (field_q, field_u)


def draw_maps(key, part):
    noise_key = jax.random.fold_in(key, 3)
    noise = jnp.clip(jax.random.normal(noise_key, (2 * SIMS, SIDE, SIDE), jnp.float32), -5.0, 5.0)
    fields = []
    for sky in range(SIMS):
        field_q, field_u = sky_pair(jax.random.fold_in(key, 100 + sky))
        fields.append(field_q)
        fields.append(field_u)
    return jnp.clip(noise + jnp.stack(fields), -12.0, 12.0)


def with_ends(values, rng, smallest, top_value):
    index_at = [jax.random.randint(jax.random.fold_in(rng, axis), (), 0, length) for axis, length in enumerate(values.shape)]
    longest = values.shape.index(max(values.shape))
    beside = index_at[:longest] + [(index_at[longest] + 1) % values.shape[longest]] + index_at[longest + 1:]
    return values.at[tuple(index_at)].set(smallest).at[tuple(beside)].set(top_value)


def setup_inputs(seed: int = 0) -> dict:
    splits = jax.random.split(jax.random.key(seed), 4)
    maps = draw_maps(jax.random.fold_in(splits[3], 71), 0)
    mask = with_ends((jax.random.randint(splits[1], (SIDE, SIDE), 0, 4) < 3).astype(jnp.int32), jax.random.fold_in(splits[1], 1), 0, 1)
    bins = draw_bins(jax.random.fold_in(splits[3], 71), 0)
    return dict(maps=maps, mask=mask, bins=bins)


def reference(maps, mask, bins):
    extent = maps.shape[1]
    weight = mask.astype(jnp.float32)
    indices = jnp.arange(extent, dtype=jnp.int32)
    signed = jnp.where(indices >= extent // 2, indices - extent, indices).astype(jnp.float32)
    freq_y = signed[:, None]
    freq_x = signed[None, :]
    radius = jnp.maximum(freq_x * freq_x + freq_y * freq_y, 1.0)
    cos_twice = (freq_x * freq_x - freq_y * freq_y) / radius
    sin_twice = 2.0 * freq_x * freq_y / radius
    inv_area = 1.0 / (extent * extent)
    flat_bins = bins.reshape(-1)

    def one_sky(couple):
        spec_q = jnp.fft.fft2(couple[0] * weight)
        spec_u = jnp.fft.fft2(couple[1] * weight)
        q_real = jnp.real(spec_q).astype(jnp.float32)
        q_imag = jnp.imag(spec_q).astype(jnp.float32)
        u_real = jnp.real(spec_u).astype(jnp.float32)
        u_imag = jnp.imag(spec_u).astype(jnp.float32)
        e_real = cos_twice * q_real + sin_twice * u_real
        e_imag = cos_twice * q_imag + sin_twice * u_imag
        b_real = -sin_twice * q_real + cos_twice * u_real
        b_imag = -sin_twice * q_imag + cos_twice * u_imag
        powers = jnp.stack([(e_real * e_real + e_imag * e_imag) * inv_area, (b_real * b_real + b_imag * b_imag) * inv_area, (e_real * b_real + e_imag * b_imag) * inv_area])
        rounded = lax.optimization_barrier(powers.astype(jnp.bfloat16)).astype(jnp.float32)
        return jax.vmap(lambda values: jax.ops.segment_sum(values.reshape(-1), flat_bins, num_segments=NBINS))(rounded)
    sums = lax.map(one_sky, maps.reshape(SIMS, 2, extent, extent))
    auto = NBINS / (extent * extent)
    cross = math.sqrt(auto)
    factors = jnp.array([auto, auto, cross], jnp.float32)[None, :, None]
    return sums * factors
```

```python
import functools
import math

import jax
import jax.numpy as jnp
import numpy as np
from jax import lax
from jax.experimental import pallas as pl
from jax.experimental.pallas import tpu as pltpu
from jax.sharding import Mesh
from jax.sharding import PartitionSpec as P

NBINS = 1024
SIDE = 4096
MESH = pl.DeviceIdType.MESH
BF = jnp.bfloat16
F32 = jnp.float32
VMEM = pltpu.VMEM
ZSTRIDE = 136


def halves(table):
    high = np.asarray(table, np.float32).astype(BF)
    low = (np.asarray(table, np.float64) - high.astype(np.float64)).astype(np.float32).astype(BF)
    return high, low


def angle(first, second, period):
    return 2.0 * np.pi * ((np.asarray(first)[:, None] * np.asarray(second)[None, :]) % period) / period


def row_tables():
    first = angle(np.arange(32), np.arange(32), 32)
    stage = np.concatenate([np.cos(first), -np.sin(first)], 0)
    first_high, first_low = halves(np.kron(stage, np.eye(8)))
    turn = angle(np.arange(32), np.arange(128), 4096)
    turn_cos = np.repeat(np.cos(turn)[:, None, :], 8, 1).astype(np.float32)
    turn_sin = np.repeat(-np.sin(turn)[:, None, :], 8, 1).astype(np.float32)
    last = angle(np.arange(64), np.arange(128), 128)
    cos, sin = np.cos(last), np.sin(last)
    last_high, last_low = halves(np.block([[cos, sin], [-sin, cos]]))
    alternate = np.zeros((16, 256), np.float32)
    alternate[0, :128] = 1.0 - 2.0 * (np.arange(128) % 2)
    return first_high, first_low, turn_cos, turn_sin, last_high, last_low, alternate.astype(BF)


def column_tables():
    first = angle(np.arange(64), np.arange(64), 64)
    cos, sin = np.cos(first), np.sin(first)
    high, low = halves(np.block([[cos, sin], [-sin, cos]]))
    doubled = np.concatenate([high, high], 1)
    turn = angle(np.arange(64), np.arange(64), 4096)
    turn_cos = np.tile(np.cos(turn), (1, 2)).astype(np.float32)
    turn_sin = np.tile(-np.sin(turn), (1, 2)).astype(np.float32)
    cos2, sin2 = np.kron(np.eye(2), cos), np.kron(np.eye(2), sin)
    last_high, last_low = halves(np.block([[cos2, -sin2], [sin2, cos2]]))
    return doubled, low, turn_cos, turn_sin, last_high, last_low


def split(values):
    high = values.astype(BF)
    return high, (values - high.astype(F32)).astype(BF)


def dot(left, right):
    return jnp.dot(left, right, preferred_element_type=F32)


def dot_nt(left, right):
    return lax.dot_general(left, right, (((1,), (1,)), ((), ())), preferred_element_type=F32)


def slot_of(block):
    group, part = block // 4, block % 4
    return (part % 2) * 64 + (group if part < 2 else 63 - group)


def row_kernel(maps, mask, t1h, t1l, twc, tws, t2h, t2l, alt, out, yh, yl, z):
    for g in range(0, 8, 2):
        pair = []
        for k in (g, g + 1):
            rows = maps[0, 8 * k : 8 * k + 8, :] * mask[8 * k : 8 * k + 8, :].astype(F32)
            pair.append(jnp.concatenate([rows[:, 128 * a : 128 * a + 128] for a in range(32)], 0))
        high, low = split(jnp.concatenate(pair, 1))
        got = dot(t1h[...], high) + dot(t1h[...], low) + dot(t1l[...], high)
        real = got[:256].reshape(32, 8, 256)
        imag = got[256:].reshape(32, 8, 256)
        for k in (0, 1):
            re, im = real[:, :, 128 * k : 128 * k + 128], imag[:, :, 128 * k : 128 * k + 128]
            pair[k] = (re * twc[...] - im * tws[...], re * tws[...] + im * twc[...])
        for part in (0, 1):
            high, low = split(jnp.concatenate([pair[0][part], pair[1][part]], 1))
            yh[:, 8 * g : 8 * g + 16, 128 * part : 128 * part + 128] = high
            yl[:, 8 * g : 8 * g + 16, 128 * part : 128 * part + 128] = low
    for jj in range(8):
        high = yh[4 * jj : 4 * jj + 4].reshape(256, 256)
        low = yl[4 * jj : 4 * jj + 4].reshape(256, 256)
        got = dot_nt(t2h[...], high) + dot_nt(t2h[...], low) + dot_nt(t2l[...], high)
        for k in (0, 1):
            z[ZSTRIDE * (2 * jj + k) : ZSTRIDE * (2 * jj + k) + 128, :] = got[:, 128 * k : 128 * k + 128]
        if jj == 0:
            edge = dot_nt(alt[...], high) + dot_nt(alt[...], low)
            lane = lax.broadcasted_iota(jnp.int32, (8, 128), 1)
            row = lax.broadcasted_iota(jnp.int32, (8, 128), 0)
            old = got[64:72, :128]
            z[64:72, :] = jnp.where((row == 0) & (lane < 64), edge[0:8, :128], old)
    for block in range(128):
        q2, h = block // 2, block % 2
        for ri in (0, 1):
            start = ZSTRIDE * 8 * h + 64 * ri + q2
            out[slot_of(block), 8 * ri : 8 * ri + 8, :] = z[pl.ds(start, 8, stride=ZSTRIDE), :]


def row_blocks(maps, mask):
    return pl.pallas_call(
        row_kernel,
        out_shape=jax.ShapeDtypeStruct((128, 16, 128), F32),
        in_specs=[pl.BlockSpec(memory_space=VMEM)] * 9,
        out_specs=pl.BlockSpec(memory_space=VMEM),
        scratch_shapes=[VMEM((32, 64, 256), BF), VMEM((32, 64, 256), BF), VMEM((16 * ZSTRIDE, 128), F32)],
        compiler_params=pltpu.CompilerParams(vmem_limit_bytes=40 << 20),
        name="row_dft",
    )(maps, mask, *row_tables())


def exchange_kernel(x, o, send_sem, recv_sem):
    r, s, m = lax.axis_index("rows"), lax.axis_index("sky"), lax.axis_index("pair")
    me = m * 64 + r

    def target(i):
        t = lax.rem(me + i, 128)
        return t, {"rows": lax.rem(t, 64), "sky": s, "pair": t // 64}

    barrier = pltpu.get_barrier_semaphore()

    def greet(i, carry):
        _, where = target(i)
        pl.semaphore_signal(barrier, inc=1, device_id=where, device_id_type=MESH)
        return carry

    lax.fori_loop(1, 128, greet, 0)
    pl.semaphore_wait(barrier, 127)

    def send(i, carry):
        t, where = target(i)
        pltpu.make_async_remote_copy(
            src_ref=x.at[t], dst_ref=o.at[me], send_sem=send_sem, recv_sem=recv_sem,
            device_id=where, device_id_type=MESH,
        ).start()
        return carry

    lax.fori_loop(1, 128, send, 0)
    o[me] = x[me]
    pltpu.make_async_copy(x.at[pl.ds(0, 127)], o.at[pl.ds(0, 127)], send_sem).wait()
    pltpu.make_async_copy(x.at[pl.ds(0, 127)], o.at[pl.ds(0, 127)], recv_sem).wait()


def exchange(blocks):
    return pl.pallas_call(
        exchange_kernel,
        out_shape=jax.ShapeDtypeStruct(blocks.shape, blocks.dtype),
        in_specs=[pl.BlockSpec(memory_space=VMEM)],
        out_specs=pl.BlockSpec(memory_space=VMEM),
        scratch_shapes=[pltpu.SemaphoreType.DMA, pltpu.SemaphoreType.DMA],
        compiler_params=pltpu.CompilerParams(collective_id=0, has_side_effects=True),
        name="sky_exchange",
    )(blocks)


def bins_kernel(bins, own, send, first, scr):
    r, m = lax.axis_index("rows"), lax.axis_index("pair")
    upper = (r >= 32).astype(jnp.int32)
    scr[0:4096, :] = bins[...].astype(F32)
    scr[4096:4104, :] = bins[0:8, :].astype(F32)
    row = lax.broadcasted_iota(jnp.int32, (48, 64), 0)
    col = lax.broadcasted_iota(jnp.int32, (48, 64), 1)
    offset = 2 * (row % 8) + (row // 8) % 2
    sent = row // 16
    below = 16 * m + 32 * sent + offset
    above = 32 + 32 * sent - 16 * m - offset
    wanted = jnp.where(row >= 32, jnp.where(row == 32, 0, -1), jnp.where(upper == 1, above, below))
    pick = (wanted == col).astype(F32)
    pick_high, pick_low = (32.0 * pick).astype(BF), pick.astype(BF)
    src = lax.broadcasted_iota(jnp.int32, (64, 128), 0)
    lane = lax.broadcasted_iota(jnp.int32, (64, 128), 1)
    there = jnp.where(upper == 1, 63 - src, src)
    put = [(lane == there + 64 * half).astype(F32) for half in (0, 1)]
    put_high = [(32.0 * one).astype(BF) for one in put]
    put_low = [one.astype(BF) for one in put]

    def body(k, carry):
        for u in range(4):
            p1 = 4 * k + u
            start = jnp.where(upper == 1, 64 - p1, p1)
            block = scr[pl.ds(start, 64, stride=64), :]
            high = jnp.floor(block * (1.0 / 32.0))
            low = block - 32.0 * high
            got = dot_nt(pick_high, high.astype(BF)) + dot_nt(pick_low, low.astype(BF))
            high = jnp.floor(got * (1.0 / 32.0))
            low = (got - 32.0 * high).astype(BF)
            high = high.astype(BF)
            wide = [dot(high, put_high[i]) + dot(low, put_low[i]) for i in (0, 1)]
            own[pl.ds(p1, 8, stride=64), :] = wide[0][0:8] + wide[1][8:16]
            send[pl.ds(p1, 8, stride=64), :] = wide[0][16:24] + wide[1][24:32]
            first[pl.ds(p1, 1), :] = wide[0][32:33] + wide[1][32:33]
        return carry

    lax.fori_loop(0, 16, body, 0)


def arrange_bins(bins):
    return pl.pallas_call(
        bins_kernel,
        out_shape=[
            jax.ShapeDtypeStruct((512, 128), F32),
            jax.ShapeDtypeStruct((512, 128), F32),
            jax.ShapeDtypeStruct((64, 128), F32),
        ],
        in_specs=[pl.BlockSpec(memory_space=VMEM)],
        out_specs=[pl.BlockSpec(memory_space=VMEM)] * 3,
        scratch_shapes=[VMEM((4104, 64), F32)],
        compiler_params=pltpu.CompilerParams(vmem_limit_bytes=30 << 20),
        name="bin_layout",
    )(bins)


def column_kernel(got, own, other, first, tah, tal, twc, tws, t2h, t2l, out, powers, index):
    r, m = lax.axis_index("rows"), lax.axis_index("pair")
    lower = r < 32
    block = jnp.where(lower, 4 * r + m, 4 * (63 - r) + 2 + m)
    p1 = lax.broadcasted_iota(jnp.int32, (64, 128), 0)
    lane = lax.broadcasted_iota(jnp.int32, (64, 128), 1)
    p = p1 + 64 * (lane % 64)
    second = lane // 64
    signed = jnp.where(p >= SIDE // 2, p - SIDE, p)
    back = jnp.where(p == SIDE // 2, signed, -signed)
    zero = jnp.zeros((64, 128), F32)
    out[...] = jnp.zeros_like(out)

    def spectrum(parts):
        high, low = split(jnp.concatenate([jnp.concatenate(part, 0) for part in parts], 1))
        mid = dot(tah[...], jnp.concatenate([high, low], 0)) + dot(tal[...], high)
        turned = []
        for k in (0, 1):
            re, im = mid[:64, 128 * k : 128 * k + 128], mid[64:, 128 * k : 128 * k + 128]
            turned.append(
                jnp.concatenate([re * twc[...] - im * tws[...], re * tws[...] + im * twc[...]], 1)
            )
        high, low = split(jnp.concatenate(turned, 0))
        last = dot(high, t2h[...]) + dot(low, t2h[...]) + dot(high, t2l[...])
        return last[:64, :128], last[:64, 128:], last[64:, :128], last[64:, 128:]

    def set_powers(base, fields, cos_twice, sin_twice):
        q_re, q_im, u_re, u_im = fields
        e_re = cos_twice * q_re + sin_twice * u_re
        e_im = cos_twice * q_im + sin_twice * u_im
        b_re = cos_twice * u_re - sin_twice * q_re
        b_im = cos_twice * u_im - sin_twice * q_im
        scale = 1.0 / (SIDE * SIDE)
        terms = (e_re * e_re + e_im * e_im, b_re * b_re + b_im * b_im, e_re * b_re + e_im * b_im)
        for k in range(3):
            powers[base + k] = (terms[k] * scale).astype(BF).astype(F32)

    def turn(freq_x, freq_y):
        radius = jnp.maximum(freq_x * freq_x + freq_y * freq_y, 1.0)
        return (freq_x * freq_x - freq_y * freq_y) / radius, 2.0 * freq_x * freq_y / radius

    def set_index(base, values):
        high = jnp.floor(values * (1.0 / 32.0))
        index[base] = high
        index[base + 1] = values - 32.0 * high

    want = lax.broadcasted_iota(jnp.int32, (32, 128), 0).astype(F32)
    one = jnp.ones((32, 128), F32)
    none = jnp.zeros((32, 128), F32)

    def add_up(kind):
        def body(k, carry):
            base = pl.multiple_of(8 * k, 8)
            hi, lo = index[2 * kind, pl.ds(base, 8), :], index[2 * kind + 1, pl.ds(base, 8), :]
            vals = [powers[3 * kind + c, pl.ds(base, 8), :] for c in range(3)]
            left, right = [], []
            for i in range(8):
                hot = jnp.broadcast_to(hi[i : i + 1], (32, 128)) == want
                cols = [
                    jnp.where(hot, jnp.broadcast_to(vals[c][i : i + 1], (32, 128)), none) for c in range(3)
                ]
                left.append(jnp.concatenate(cols, 0).astype(BF))
                right.append(
                    jnp.where(jnp.broadcast_to(lo[i : i + 1], (32, 128)) == want, one, none).astype(BF)
                )
            return carry + dot_nt(jnp.concatenate(left, 1), jnp.concatenate(right, 1))

        out[...] += lax.fori_loop(0, 8, body, jnp.zeros((96, 32), F32))

    def pair_of(j):
        parts = []
        for k in (0, 1):
            parts.append(
                [got[pl.ds(1024 * k + 8 * c + j, 64, stride=16), :] for c in (0, 1)]
            )
        return parts

    def columns(j, carry):
        fields = spectrum(pair_of(j))
        freq_x = (16 * block + 2 * j + second).astype(F32)
        cos_twice, sin_twice = turn(freq_x, signed.astype(F32))
        set_powers(0, fields, cos_twice, sin_twice)
        set_powers(3, fields, cos_twice, jnp.where(p == SIDE // 2, -sin_twice, sin_twice))
        rows = pl.ds(pl.multiple_of(64 * j, 64), 64)
        mine, theirs = own[rows, :], other[rows, :]
        ahead = jnp.where(lower, mine, theirs)
        mirror = jnp.where(lower, theirs, mine)
        edge = (j == 0) & lower & (m == 0)
        mirror = jnp.where(edge & (second == 0), first[...], mirror)
        packed = edge & (r == 0) & (second == 0)
        set_index(0, jnp.where(packed, -1.0, ahead))
        set_index(2, jnp.where(packed, -1.0, mirror))
        add_up(0)
        add_up(1)
        return carry

    lax.fori_loop(0, 8, columns, 0)

    parts = []
    for re, im in pair_of(0):
        parts.append([jnp.where(second == 0, re, pltpu.roll(im, 64, 1)), zero])
    fields = spectrum(parts)
    freq_x = jnp.where(second == 0, 0.0, -(SIDE // 2) * 1.0)
    freq_y = jnp.where(second == 0, signed, back).astype(F32)
    set_powers(0, fields, *turn(freq_x, freq_y))
    special = jnp.where(second == 0, own[0:64, :], first[...])
    set_index(0, jnp.where((r == 0) & (m == 0), special, -1.0))
    add_up(0)


def binned(blocks, own, other, first):
    return pl.pallas_call(
        column_kernel,
        out_shape=jax.ShapeDtypeStruct((96, 32), F32),
        in_specs=[pl.BlockSpec(memory_space=VMEM)] * 10,
        out_specs=pl.BlockSpec(memory_space=VMEM),
        scratch_shapes=[VMEM((6, 64, 128), F32), VMEM((4, 64, 128), F32)],
        compiler_params=pltpu.CompilerParams(vmem_limit_bytes=40 << 20),
        name="column_bins",
    )(blocks.reshape(2048, 128), own, other, first, *column_tables())


def total_kernel(part, out, stage, seen_a, seen_b, seen_c, send_sem, recv_sem):
    r, s, m = lax.axis_index("rows"), lax.axis_index("sky"), lax.axis_index("pair")
    low, high = lax.rem(r, 8), r // 8
    rep = 2 * s + m
    peers = [[], [], []]
    for i in range(1, 8):
        peers[0].append({"rows": high * 8 + lax.rem(low + i, 8), "sky": s, "pair": m})
        peers[1].append({"rows": lax.rem(high + i, 8) * 8 + low, "sky": s, "pair": m})
    for i in range(1, 4):
        other = lax.rem(rep + i, 4)
        peers[2].append({"rows": r, "sky": other // 2, "pair": lax.rem(other, 2)})
    barrier = pltpu.get_barrier_semaphore()
    for group in peers:
        for where in group:
            pl.semaphore_signal(barrier, inc=1, device_id=where, device_id_type=MESH)
    pl.semaphore_wait(barrier, 17)

    def phase(k, src, seen, me):
        count = len(peers[k])
        for where in peers[k]:
            pltpu.make_async_remote_copy(
                src_ref=src, dst_ref=seen.at[me], send_sem=send_sem.at[k], recv_sem=recv_sem.at[k],
                device_id=where, device_id_type=MESH,
            ).start()
        seen[me] = src[...]
        whole = seen.at[pl.ds(0, count)]
        pltpu.make_async_copy(whole, whole, send_sem.at[k]).wait()
        pltpu.make_async_copy(whole, whole, recv_sem.at[k]).wait()

    phase(0, part, seen_a, low)
    stage[0] = jnp.sum(seen_a[...], axis=0)
    phase(1, stage.at[0], seen_b, high)
    stage[1] = jnp.sum(seen_b[...], axis=0)
    phase(2, stage.at[1], seen_c, rep)
    auto = NBINS / (SIDE * SIDE)
    row = lax.broadcasted_iota(jnp.int32, (24, 128), 0)
    factors = jnp.where(row < 16, auto, math.sqrt(auto))
    for sky in (0, 1):
        out[sky] = (seen_c[2 * sky] + seen_c[2 * sky + 1]) * factors


def totals(part):
    return pl.pallas_call(
        total_kernel,
        out_shape=jax.ShapeDtypeStruct((2, 24, 128), F32),
        in_specs=[pl.BlockSpec(memory_space=VMEM)],
        out_specs=pl.BlockSpec(memory_space=VMEM),
        scratch_shapes=[
            VMEM((2, 24, 128), F32),
            VMEM((8, 24, 128), F32),
            VMEM((8, 24, 128), F32),
            VMEM((4, 24, 128), F32),
            pltpu.SemaphoreType.DMA((3,)),
            pltpu.SemaphoreType.DMA((3,)),
        ],
        compiler_params=pltpu.CompilerParams(collective_id=1, has_side_effects=True),
        name="sky_totals",
    )(part)


def on_device(maps, mask, bins):
    own, send, first = arrange_bins(bins)
    other = lax.ppermute(send, "rows", [(i, 63 - i) for i in range(64)])
    column = lax.ppermute(first, "rows", [(32, 0)] + [(i, 64 - i) for i in range(33, 64)])
    blocks = exchange(row_blocks(maps, mask))
    part = binned(blocks, own, other, column)
    return totals(part.reshape(24, 128)).reshape(2, 3, NBINS)


def solution(mesh):
    parted = Mesh(mesh.devices.reshape(mesh.shape["rows"], 2, 2), ("rows", "sky", "pair"))
    placed = (P(("sky", "pair"), "rows", None), P("rows", None), P(None, "rows"))
    return jax.shard_map(on_device, mesh=parted, in_specs=placed, out_specs=P(), check_vma=False)
```

```python
import functools
import math

import jax
import jax.numpy as jnp
import numpy as np
from jax import lax
from jax.experimental import pallas as pl
from jax.experimental.pallas import tpu as pltpu
from jax.sharding import Mesh
from jax.sharding import PartitionSpec as P

NBINS = 1024
SIDE = 4096
MESH = pl.DeviceIdType.MESH
BF = jnp.bfloat16
F32 = jnp.float32
VMEM = pltpu.VMEM
STEP = 72
CHUNKS = 2
PAIRS = 8 // CHUNKS
LINES = 2 * PAIRS
UNROLL = 64


def halves(table):
    high = np.asarray(table, np.float32).astype(BF)
    low = (np.asarray(table, np.float64) - high.astype(np.float64)).astype(np.float32).astype(BF)
    return high, low


def angle(first, second, period):
    return 2.0 * np.pi * ((np.asarray(first)[:, None] * np.asarray(second)[None, :]) % period) / period


def row_tables():
    first = angle(np.arange(32), np.arange(32), 32)
    stage = np.concatenate([np.cos(first), -np.sin(first)], 0)
    first_high, first_low = halves(np.kron(stage, np.eye(8)))
    turn = angle(np.arange(32), np.arange(128), 4096)
    turn_cos = np.repeat(np.cos(turn)[:, None, :], 8, 1).astype(np.float32)
    turn_sin = np.repeat(-np.sin(turn)[:, None, :], 8, 1).astype(np.float32)
    last = angle(np.arange(64), np.arange(128), 128)
    cos, sin = np.cos(last), np.sin(last)
    last_high, last_low = halves(np.block([[cos, sin], [-sin, cos]]))
    alternate = np.zeros((16, 256), np.float32)
    alternate[0, :128] = 1.0 - 2.0 * (np.arange(128) % 2)
    return first_high, first_low, turn_cos, turn_sin, last_high, last_low, alternate.astype(BF)


def column_tables():
    first = angle(np.arange(64), np.arange(64), 64)
    cos, sin = np.cos(first), np.sin(first)
    high, low = halves(np.block([[cos, sin], [-sin, cos]]))
    doubled = np.concatenate([high, high], 1)
    turn = angle(np.arange(128), np.arange(64), 4096)
    turn_cos = np.tile(np.cos(turn), (1, 2)).astype(np.float32)
    turn_sin = np.tile(-np.sin(turn), (1, 2)).astype(np.float32)
    last = angle(np.arange(32), np.arange(64), 32)
    cos, sin = np.cos(last), np.sin(last)
    none = np.zeros_like(cos)
    last_high, last_low = halves(
        np.block(
            [
                [cos, none, sin, none],
                [-sin, none, cos, none],
                [none, cos, none, sin],
                [none, -sin, none, cos],
            ]
        )
    )
    flip = np.zeros((128, 128), np.float32)
    flip[(128 - np.arange(128)) % 128, np.arange(128)] = 1.0
    return doubled, low, turn_cos, turn_sin, last_high, last_low, flip.astype(BF)


def split(values):
    high = values.astype(BF)
    return high, (values - high.astype(F32)).astype(BF)


def dot(left, right):
    return jnp.dot(left, right, preferred_element_type=F32)


def dot_nt(left, right):
    return lax.dot_general(left, right, (((1,), (1,)), ((), ())), preferred_element_type=F32)


def slot_of(block):
    group, part = block // 4, block % 4
    return (part % 2) * 64 + (group if part < 2 else 63 - group)


def spread(line):
    tile = jnp.broadcast_to(line, (8, 128))
    return jnp.concatenate([tile, tile], 0).astype(BF)


def kernel(
    maps, mask, bins, t1h, t1l, twc, tws, t2h, t2l, alt, tah, tal, cwc, cws, tbh, tbl, flip,
    out,
    yh, yl, z, x, o, ahead, mirror, ahead_hi, ahead_lo, mirror_hi, mirror_lo, powers, acc,
    stage, seen_a, seen_b, seen_c, send_sem, recv_sem, bin_send, bin_recv, bin_here, sum_send, sum_recv,
):
    r, s, m = lax.axis_index("rows"), lax.axis_index("sky"), lax.axis_index("pair")
    me = m * 64 + r
    lower = r < 32
    low_row, high_row = lax.rem(r, 8), r // 8
    rep = 2 * s + m

    def target(i):
        t = lax.rem(me + i, 128)
        return t, {"rows": lax.rem(t, 64), "sky": s, "pair": t // 64}

    barrier = pltpu.get_barrier_semaphore()

    def greet(i, carry):
        _, where = target(i)
        pl.semaphore_signal(barrier, inc=1, device_id=where, device_id_type=MESH)
        return carry

    lax.fori_loop(1, 128, greet, 0)
    for pair in (0, 1):
        pl.semaphore_signal(
            barrier, inc=1, device_id={"rows": r, "sky": 1 - s, "pair": pair}, device_id_type=MESH
        )

    @pl.when(lower)
    def _():
        pltpu.make_async_copy(bins.at[pl.ds(16 * m, 16)], ahead, bin_here).start()

    @pl.when(jnp.logical_not(lower))
    def _():
        pltpu.make_async_copy(bins.at[pl.ds(16 - 16 * m, 16)], mirror.at[pl.ds(0, 16)], bin_here).start()
        pltpu.make_async_copy(bins.at[pl.ds(32 - 16 * m, 8)], mirror.at[pl.ds(16, 8)], bin_here).start()

    for g in range(0, 8, 2):
        pair = []
        for k in (g, g + 1):
            rows = maps[0, 8 * k : 8 * k + 8, :] * mask[8 * k : 8 * k + 8, :].astype(F32)
            pair.append(jnp.concatenate([rows[:, 128 * a : 128 * a + 128] for a in range(32)], 0))
        high, low = split(jnp.concatenate(pair, 1))
        got = dot(t1h[...], high) + dot(t1h[...], low) + dot(t1l[...], high)
        real = got[:256].reshape(32, 8, 256)
        imag = got[256:].reshape(32, 8, 256)
        for k in (0, 1):
            re, im = real[:, :, 128 * k : 128 * k + 128], imag[:, :, 128 * k : 128 * k + 128]
            pair[k] = (re * twc[...] - im * tws[...], re * tws[...] + im * twc[...])
        for part in (0, 1):
            high, low = split(jnp.concatenate([pair[0][part], pair[1][part]], 1))
            yh[:, 8 * g : 8 * g + 16, 128 * part : 128 * part + 128] = high
            yl[:, 8 * g : 8 * g + 16, 128 * part : 128 * part + 128] = low

    def second_stage(jj):
        high = yh[4 * jj : 4 * jj + 4].reshape(256, 256)
        low = yl[4 * jj : 4 * jj + 4].reshape(256, 256)
        got = dot_nt(t2h[...], high) + dot_nt(t2h[...], low) + dot_nt(t2l[...], high)
        for k in (0, 1):
            for ri in (0, 1):
                start = STEP * (2 * (2 * jj + k) + ri)
                z[start : start + 64, :] = got[64 * ri : 64 * ri + 64, 128 * k : 128 * k + 128]
        if jj == 0:
            edge = dot_nt(alt[...], high) + dot_nt(alt[...], low)
            lane = lax.broadcasted_iota(jnp.int32, (8, 128), 1)
            row = lax.broadcasted_iota(jnp.int32, (8, 128), 0)
            z[STEP : STEP + 8, :] = jnp.where((row == 0) & (lane < 64), edge[0:8, :128], got[64:72, :128])

    def send_chunk(c):
        def send(i, carry):
            t, where = target(i)
            pltpu.make_async_remote_copy(
                src_ref=x.at[c, t], dst_ref=o.at[c, me], send_sem=send_sem.at[c], recv_sem=recv_sem.at[c],
                device_id=where, device_id_type=MESH,
            ).start()
            return carry

        lax.fori_loop(1, 128, send, 0)
        o[c, me] = x[c, me]

    partner = {"rows": 63 - r, "sky": s, "pair": m}
    for c in range(CHUNKS):
        for h in (0, 1):
            for jj in range((8 * h + PAIRS * c) // 2, (8 * h + PAIRS * (c + 1)) // 2):
                second_stage(jj)
        for block in range(128):
            q2, h = block // 2, block % 2
            start = STEP * 2 * (8 * h + PAIRS * c) + q2
            x[c, slot_of(block)] = z[pl.ds(start, LINES, stride=STEP), :]
        if c == 0:
            pl.semaphore_wait(barrier, 129)
        send_chunk(c)
        if c == 0:

            @pl.when(lower)
            def _():
                pltpu.make_async_remote_copy(
                    src_ref=bins.at[pl.ds(32 + 16 * m, 16)], dst_ref=ahead, send_sem=bin_send,
                    recv_sem=bin_recv, device_id=partner, device_id_type=MESH,
                ).start()

            @pl.when(jnp.logical_not(lower))
            def _():
                pltpu.make_async_remote_copy(
                    src_ref=bins.at[pl.ds(48 - 16 * m, 16)], dst_ref=mirror.at[pl.ds(0, 16)],
                    send_sem=bin_send, recv_sem=bin_recv, device_id=partner, device_id_type=MESH,
                ).start()
                beside = lax.rem(64 - r, 32) * (1 - m) + (63 - r) * m
                pltpu.make_async_remote_copy(
                    src_ref=bins.at[pl.ds(48 * m, 8)], dst_ref=mirror.at[pl.ds(16, 8)],
                    send_sem=bin_send, recv_sem=bin_recv,
                    device_id={"rows": beside, "sky": s, "pair": m}, device_id_type=MESH,
                ).start()

    @pl.when(lower)
    def _():
        pltpu.make_async_copy(bins.at[pl.ds(0, 16)], ahead, bin_here).wait()
        pltpu.make_async_copy(bins.at[pl.ds(0, 24)], mirror, bin_recv).wait()
        pltpu.make_async_copy(bins.at[pl.ds(0, 16)], ahead, bin_send).wait()

    @pl.when(jnp.logical_not(lower))
    def _():
        pltpu.make_async_copy(bins.at[pl.ds(0, 24)], mirror, bin_here).wait()
        pltpu.make_async_copy(bins.at[pl.ds(0, 16)], ahead, bin_recv).wait()
        pltpu.make_async_copy(bins.at[pl.ds(0, 24)], mirror, bin_send).wait()

    first_block = (r == 0) & (m == 0)
    none_first = jnp.where(first_block, -1.0, 0.0)
    for src, hi, lo in ((ahead, ahead_hi, ahead_lo), (mirror, mirror_hi, mirror_lo)):
        whole = src[...]
        tiles = [whole[:, 128 * i : 128 * i + 128] for i in range(32)]
        whole = jnp.concatenate(tiles, 0)
        hi[...] = (whole // 32).astype(F32)
        lo[...] = (whole % 32).astype(F32)

    line = lax.broadcasted_iota(jnp.int32, (32, 128), 0)
    lane = lax.broadcasted_iota(jnp.int32, (32, 128), 1)
    p = lane + 128 * line
    signed = jnp.where(p >= SIDE // 2, p - SIDE, p)
    back = jnp.where(p == SIDE // 2, signed, -signed)
    half = lax.broadcasted_iota(jnp.int32, (64, 128), 1) // 64
    block = jnp.where(lower, 4 * r + m, 4 * (63 - r) + 2 + m)
    acc[...] = jnp.zeros_like(acc)

    def spectrum(parts):
        high, low = split(jnp.concatenate([jnp.concatenate(part, 0) for part in parts], 1))
        mid = dot(tah[...], jnp.concatenate([high, low], 0)) + dot(tal[...], high)
        turned = []
        for k in (0, 1):
            re, im = mid[:64, 128 * k : 128 * k + 128], mid[64:, 128 * k : 128 * k + 128]
            re, im = jnp.concatenate([re, re], 0), jnp.concatenate([im, im], 0)
            turned.append(
                jnp.concatenate([re * cwc[...] - im * cws[...], re * cws[...] + im * cwc[...]], 1)
            )
        high, low = split(jnp.concatenate(turned, 0))
        last = dot_nt(tbh[...], high) + dot_nt(tbh[...], low) + dot_nt(tbl[...], high)
        return [
            (last[64 * c : 64 * c + 32, :128], last[64 * c + 32 : 64 * c + 64, :128],
             last[64 * c : 64 * c + 32, 128:], last[64 * c + 32 : 64 * c + 64, 128:])
            for c in (0, 1)
        ]

    def power_of(fields, freq_x, freq_y):
        radius = jnp.maximum(freq_x * freq_x + freq_y * freq_y, 1.0)
        cos_twice = (freq_x * freq_x - freq_y * freq_y) / radius
        sin_twice = 2.0 * freq_x * freq_y / radius
        q_re, q_im, u_re, u_im = fields
        e_re = cos_twice * q_re + sin_twice * u_re
        e_im = cos_twice * q_im + sin_twice * u_im
        b_re = cos_twice * u_re - sin_twice * q_re
        b_im = cos_twice * u_im - sin_twice * q_im
        scale = 1.0 / (SIDE * SIDE)
        terms = (e_re * e_re + e_im * e_im, b_re * b_re + b_im * b_im, e_re * b_re + e_im * b_im)
        return jnp.concatenate([(term * scale).astype(BF) for term in terms], 0)

    def reversed_lines(values):
        turned = dot(values, flip[...])
        parts = [turned[32 * k : 32 * k + 32] for k in range(3)]
        return jnp.concatenate([jnp.where(lane == 0, pltpu.roll(part, 31, 0), part) for part in parts], 0)

    want = lax.broadcasted_iota(jnp.int32, (32, 128), 0).astype(F32).astype(BF)
    wants = (want[:16], want[16:])
    one, none = jnp.ones((16, 128), BF), jnp.zeros((16, 128), BF)

    def add_up(items):
        total = acc[:, 0:32]
        for start in range(0, len(items), UNROLL):
            left, right = [], []
            for kind, c, row, hi, lo in items[start : start + UNROLL]:
                hot, cold = spread(hi(row)), spread(lo(row))
                vals = [spread(powers[kind, c, 32 * k + row : 32 * k + row + 1, :]) for k in range(3)]
                left.append(
                    jnp.concatenate([jnp.where(hot == w, val, none) for val in vals for w in wants], 0)
                )
                right.append(jnp.concatenate([jnp.where(cold == w, one, none) for w in wants], 0))
            total = total + dot_nt(jnp.concatenate(left, 1), jnp.concatenate(right, 1))
        acc[:, 0:32] = total

    def lines_of(ref, index, flipped):
        def get(row):
            at = 31 - row if flipped else row
            return ref[pl.ds(ref.shape[0] // 32 * at + index, 1), :]

        return get

    def pair_of(c, j):
        return [
            [o[c, pl.ds(64 * k, 64), pl.ds(2 * j + ri, 1), :].reshape(64, 128) for ri in (0, 1)] for k in (0, 1)
        ]

    def run_pair(c, j):
        fields = spectrum(pair_of(c, j))
        freq_y = signed.astype(F32)
        items = []
        for k in (0, 1):
            column = 2 * (PAIRS * c + j) + k
            freq_x = (16 * block + column).astype(F32)
            powers[0, k] = power_of(fields[k], freq_x, freq_y).astype(F32)
            powers[1, k] = reversed_lines(power_of(fields[k], -freq_x, back.astype(F32)))
            for row in range(32):
                items.append((0, k, row, lines_of(ahead_hi, column, False), lines_of(ahead_lo, column, False)))
        for k in (0, 1):
            column = 2 * (PAIRS * c + j) + k
            for row in range(32):
                items.append(
                    (1, k, row, lines_of(mirror_hi, 16 - column, True), lines_of(mirror_lo, 16 - column, True))
                )
        add_up(items)

    for c in range(CHUNKS):
        pltpu.make_async_copy(x.at[c, pl.ds(0, 127)], o.at[c, pl.ds(0, 127)], recv_sem.at[c]).wait()
        if c == 0:

            @pl.when(first_block)
            def _():
                parts = []
                for re, im in pair_of(0, 0):
                    parts.append([jnp.where(half == 0, re, pltpu.roll(im, 64, 1)), jnp.zeros((64, 128), F32)])
                fields = spectrum(parts)
                powers[0, 0] = power_of(fields[0], jnp.zeros((32, 128), F32), signed.astype(F32)).astype(F32)
                last = power_of(fields[1], jnp.full((32, 128), -(SIDE // 2) * 1.0, F32), back.astype(F32))
                powers[0, 1] = reversed_lines(last)
                items = [(0, 0, row, lines_of(ahead_hi, 0, False), lines_of(ahead_lo, 0, False)) for row in range(32)]
                items += [
                    (0, 1, row, lines_of(mirror_hi, 16, True), lines_of(mirror_lo, 16, True)) for row in range(32)
                ]
                add_up(items)
                ahead_hi[pl.ds(0, 32, stride=16), :] = jnp.full((32, 128), -1.0, F32)
                mirror_hi[pl.ds(16, 32, stride=24), :] = jnp.full((32, 128), -1.0, F32)

        def body(j, carry):
            run_pair(c, j)
            return carry

        lax.fori_loop(0, PAIRS, body, 0)

    for c in range(CHUNKS):
        pltpu.make_async_copy(x.at[c, pl.ds(0, 127)], o.at[c, pl.ds(0, 127)], send_sem.at[c]).wait()

    wide = lax.broadcasted_iota(jnp.int32, (24, 128), 1) // 32
    part = jnp.zeros((24, 128), F32)
    for u in range(4):
        piece = acc[pl.ds(u, 24, stride=4), :]
        part = jnp.where(wide == u, piece if u == 0 else pltpu.roll(piece, 32 * u, 1), part)
    stage[0] = part
    peers = [[], [], []]
    for i in range(1, 8):
        peers[0].append({"rows": high_row * 8 + lax.rem(low_row + i, 8), "sky": s, "pair": m})
        peers[1].append({"rows": lax.rem(high_row + i, 8) * 8 + low_row, "sky": s, "pair": m})
    for i in range(1, 4):
        other = lax.rem(rep + i, 4)
        peers[2].append({"rows": r, "sky": other // 2, "pair": lax.rem(other, 2)})

    def phase(k, seen, here):
        count = len(peers[k])
        for where in peers[k]:
            pltpu.make_async_remote_copy(
                src_ref=stage.at[k], dst_ref=seen.at[here], send_sem=sum_send.at[k],
                recv_sem=sum_recv.at[k], device_id=where, device_id_type=MESH,
            ).start()
        seen[here] = stage[k]
        some = seen.at[pl.ds(0, count)]
        pltpu.make_async_copy(some, some, sum_send.at[k]).wait()
        pltpu.make_async_copy(some, some, sum_recv.at[k]).wait()

    phase(0, seen_a, low_row)
    stage[1] = jnp.sum(seen_a[...], axis=0)
    phase(1, seen_b, high_row)
    stage[2] = jnp.sum(seen_b[...], axis=0)
    phase(2, seen_c, rep)
    auto = NBINS / (SIDE * SIDE)
    for sky in (0, 1):
        whole = seen_c[2 * sky] + seen_c[2 * sky + 1]
        for k in range(3):
            for i in range(8):
                line_of = whole[8 * k + i : 8 * k + i + 1, :] * (auto if k < 2 else math.sqrt(auto))
                out[k, sky : sky + 1, 128 * i : 128 * i + 128] = line_of


def on_device(maps, mask, bins):
    tables = row_tables() + column_tables()
    here = pl.BlockSpec(memory_space=VMEM)
    there = pl.BlockSpec(memory_space=pl.ANY)
    dma = pltpu.SemaphoreType.DMA
    sums = pl.pallas_call(
        kernel,
        out_shape=jax.ShapeDtypeStruct((3, 2, NBINS), F32),
        in_specs=[here, here, there] + [here] * len(tables),
        out_specs=here,
        scratch_shapes=[
            VMEM((32, 64, 256), BF),
            VMEM((32, 64, 256), BF),
            VMEM((32 * STEP, 128), F32),
            VMEM((CHUNKS, 128, LINES, 128), F32),
            VMEM((CHUNKS, 128, LINES, 128), F32),
            VMEM((16, SIDE), jnp.int32),
            VMEM((24, SIDE), jnp.int32),
            VMEM((16 * 32, 128), F32),
            VMEM((16 * 32, 128), F32),
            VMEM((24 * 32, 128), F32),
            VMEM((24 * 32, 128), F32),
            VMEM((2, 2, 96, 128), F32),
            VMEM((96, 128), F32),
            VMEM((3, 24, 128), F32),
            VMEM((8, 24, 128), F32),
            VMEM((8, 24, 128), F32),
            VMEM((4, 24, 128), F32),
            dma((CHUNKS,)),
            dma((CHUNKS,)),
            dma,
            dma,
            dma,
            dma((3,)),
            dma((3,)),
        ],
        compiler_params=pltpu.CompilerParams(
            collective_id=0, has_side_effects=True, vmem_limit_bytes=48 << 20
        ),
        name="sky_spectra",
    )(maps, mask, bins.T, *tables)
    return jnp.transpose(sums, (1, 0, 2))


def solution(mesh):
    parted = Mesh(mesh.devices.reshape(mesh.shape["rows"], 2, 2), ("rows", "sky", "pair"))
    placed = (P(("sky", "pair"), "rows", None), P("rows", None), P(None, "rows"))
    return jax.shard_map(on_device, mesh=parted, in_specs=placed, out_specs=P(), check_vma=False)
```

```python
import functools
import math

import jax
import jax.numpy as jnp
import numpy as np
from jax import lax
from jax.experimental import pallas as pl
from jax.experimental.pallas import tpu as pltpu
from jax.sharding import Mesh
from jax.sharding import PartitionSpec as P

NBINS = 1024
SIDE = 4096
MESH = pl.DeviceIdType.MESH
BF = jnp.bfloat16
F32 = jnp.float32
VMEM = pltpu.VMEM
STEP = 72
CHUNKS = 4
PAIRS = 8 // CHUNKS
LINES = 2 * PAIRS
UNROLL = 64


def halves(table):
    high = np.asarray(table, np.float32).astype(BF)
    low = (np.asarray(table, np.float64) - high.astype(np.float64)).astype(np.float32).astype(BF)
    return high, low


def angle(first, second, period):
    return 2.0 * np.pi * ((np.asarray(first)[:, None] * np.asarray(second)[None, :]) % period) / period


def row_tables():
    first = angle(np.arange(32), np.arange(32), 32)
    stage = np.concatenate([np.cos(first), -np.sin(first)], 0)
    first_high, first_low = halves(np.kron(stage, np.eye(8)))
    turn = angle(np.arange(32), np.arange(128), 4096)
    turn_cos = np.repeat(np.cos(turn)[:, None, :], 8, 1).astype(np.float32)
    turn_sin = np.repeat(-np.sin(turn)[:, None, :], 8, 1).astype(np.float32)
    last = angle(np.arange(64), np.arange(128), 128)
    cos, sin = np.cos(last), np.sin(last)
    last_high, last_low = halves(np.block([[cos, sin], [-sin, cos]]))
    alternate = np.zeros((16, 256), np.float32)
    alternate[0, :128] = 1.0 - 2.0 * (np.arange(128) % 2)
    return first_high, first_low, turn_cos, turn_sin, last_high, last_low, alternate.astype(BF)


def column_tables():
    first = angle(np.arange(64), np.arange(64), 64)
    cos, sin = np.cos(first), np.sin(first)
    high, low = halves(np.block([[cos, sin], [-sin, cos]]))
    doubled = np.concatenate([high, high], 1)
    turn = angle(np.arange(128), np.arange(64), 4096)
    turn_cos = np.tile(np.cos(turn), (1, 2)).astype(np.float32)
    turn_sin = np.tile(-np.sin(turn), (1, 2)).astype(np.float32)
    last = angle(np.arange(32), np.arange(64), 32)
    cos, sin = np.cos(last), np.sin(last)
    none = np.zeros_like(cos)
    last_high, last_low = halves(
        np.block(
            [
                [cos, none, sin, none],
                [-sin, none, cos, none],
                [none, cos, none, sin],
                [none, -sin, none, cos],
            ]
        )
    )
    flip = np.zeros((128, 128), np.float32)
    flip[(128 - np.arange(128)) % 128, np.arange(128)] = 1.0
    return doubled, low, turn_cos, turn_sin, last_high, last_low, flip.astype(BF)


def split(values):
    high = values.astype(BF)
    return high, (values - high.astype(F32)).astype(BF)


def dot(left, right):
    return jnp.dot(left, right, preferred_element_type=F32)


def dot_nt(left, right):
    return lax.dot_general(left, right, (((1,), (1,)), ((), ())), preferred_element_type=F32)


def slot_of(block):
    group, part = block // 4, block % 4
    return (part % 2) * 64 + (group if part < 2 else 63 - group)


def spread(line):
    tile = jnp.broadcast_to(line, (8, 128))
    return jnp.concatenate([tile, tile], 0).astype(BF)


def kernel(*refs):
    sources, refs = refs[:16], refs[16:]
    bins, out, refs = refs[0], refs[1], refs[2:]
    held, rest = refs[:16], refs[16:]
    arrived = rest[-1]
    for i in range(16):
        pltpu.make_async_copy(sources[i], held[i], arrived.at[i]).start()

    def ready(*places):
        for i in places:
            pltpu.make_async_copy(sources[i], held[i], arrived.at[i]).wait()

    work(ready, bins, out, *held, *rest[:-1])


def work(
    ready, bins, out,
    maps, mask, t1h, t1l, twc, tws, t2h, t2l, alt, tah, tal, cwc, cws, tbh, tbl, flip,
    yh, yl, z, x, o, ahead, mirror, ahead_hi, ahead_lo, mirror_hi, mirror_lo, powers, acc,
    stage, seen_a, seen_b, seen_c, send_sem, recv_sem, bin_send, bin_recv, bin_here, sum_send, sum_recv,
):
    r, s, m = lax.axis_index("rows"), lax.axis_index("sky"), lax.axis_index("pair")
    me = m * 64 + r
    lower = r < 32
    low_row, high_row = lax.rem(r, 8), r // 8
    rep = 2 * s + m

    def target(i):
        t = lax.rem(me + i, 128)
        return t, {"rows": lax.rem(t, 64), "sky": s, "pair": t // 64}

    barrier = pltpu.get_barrier_semaphore()

    def greet(i, carry):
        _, where = target(i)
        pl.semaphore_signal(barrier, inc=1, device_id=where, device_id_type=MESH)
        return carry

    lax.fori_loop(1, 128, greet, 0)
    for pair in (0, 1):
        pl.semaphore_signal(
            barrier, inc=1, device_id={"rows": r, "sky": 1 - s, "pair": pair}, device_id_type=MESH
        )

    @pl.when(lower)
    def _():
        pltpu.make_async_copy(bins.at[pl.ds(16 * m, 16)], ahead, bin_here.at[0]).start()

    @pl.when(jnp.logical_not(lower))
    def _():
        pltpu.make_async_copy(bins.at[pl.ds(16 - 16 * m, 16)], mirror.at[pl.ds(0, 16)], bin_here.at[0]).start()
        pltpu.make_async_copy(bins.at[pl.ds(32 - 16 * m, 1)], mirror.at[pl.ds(16, 1)], bin_here.at[1]).start()

    partner = {"rows": 63 - r, "sky": s, "pair": m}

    def bins_part(k):
        def ship(source, count, place, where, sem=k):
            pltpu.make_async_remote_copy(
                src_ref=bins.at[pl.ds(source, count)], dst_ref=place, send_sem=bin_send.at[sem],
                recv_sem=bin_recv.at[sem], device_id=where, device_id_type=MESH,
            ).start()

        @pl.when(lower)
        def _():
            ship(32 + 16 * m + 8 * k, 8, ahead.at[pl.ds(8 * k, 8)], partner)

        @pl.when(jnp.logical_not(lower))
        def _():
            ship(56 - 16 * m - 8 * k, 8, mirror.at[pl.ds(8 - 8 * k, 8)], partner)
            if k == 0:
                beside = lax.rem(64 - r, 32) * (1 - m) + (63 - r) * m
                ship(48 * m, 1, mirror.at[pl.ds(16, 1)], {"rows": beside, "sky": s, "pair": m}, 2)

    def bins_ready(k):
        def wait(count, sem):
            pltpu.make_async_copy(bins.at[pl.ds(0, count)], mirror.at[pl.ds(0, count)], sem).wait()

        @pl.when(lower)
        def _():
            wait(8, bin_recv.at[k])
            wait(8, bin_send.at[k])
            if k == 0:
                wait(16, bin_here.at[0])
                wait(1, bin_recv.at[2])

        @pl.when(jnp.logical_not(lower))
        def _():
            wait(8, bin_recv.at[k])
            wait(8, bin_send.at[k])
            if k == 0:
                wait(16, bin_here.at[0])
                wait(1, bin_here.at[1])
                wait(1, bin_send.at[2])

        rows = [(ahead, ahead_hi, ahead_lo, 8 * k, 8), (mirror, mirror_hi, mirror_lo, 8 - 8 * k, 8)]
        if k == 0:
            rows.append((mirror, mirror_hi, mirror_lo, 16, 1))
        for src, hi, lo, start, count in rows:
            size = src.shape[0]
            for i in range(32):
                part = src[start : start + count, 128 * i : 128 * i + 128]
                hi[size * i + start : size * i + start + count, :] = (part >> 5).astype(F32)
                lo[size * i + start : size * i + start + count, :] = (part & 31).astype(F32)

    ready(0, 1, 2, 3, 4, 5)
    for g in range(0, 8, 2):
        pair = []
        for k in (g, g + 1):
            rows = maps[8 * k : 8 * k + 8, :] * mask[8 * k : 8 * k + 8, :].astype(F32)
            pair.append(jnp.concatenate([rows[:, 128 * a : 128 * a + 128] for a in range(32)], 0))
        high, low = split(jnp.concatenate(pair, 1))
        got = dot(t1h[...], high) + dot(t1h[...], low) + dot(t1l[...], high)
        real = got[:256].reshape(32, 8, 256)
        imag = got[256:].reshape(32, 8, 256)
        for k in (0, 1):
            re, im = real[:, :, 128 * k : 128 * k + 128], imag[:, :, 128 * k : 128 * k + 128]
            pair[k] = (re * twc[...] - im * tws[...], re * tws[...] + im * twc[...])
        for part in (0, 1):
            high, low = split(jnp.concatenate([pair[0][part], pair[1][part]], 1))
            yh[:, 8 * g : 8 * g + 16, 128 * part : 128 * part + 128] = high
            yl[:, 8 * g : 8 * g + 16, 128 * part : 128 * part + 128] = low

    def second_stage(jj):
        high = yh[4 * jj : 4 * jj + 4].reshape(256, 256)
        low = yl[4 * jj : 4 * jj + 4].reshape(256, 256)
        got = dot_nt(t2h[...], high) + dot_nt(t2h[...], low) + dot_nt(t2l[...], high)
        for k in (0, 1):
            for ri in (0, 1):
                start = STEP * (2 * (2 * jj + k) + ri)
                z[start : start + 64, :] = got[64 * ri : 64 * ri + 64, 128 * k : 128 * k + 128]
        if jj == 0:
            edge = dot_nt(alt[...], high) + dot_nt(alt[...], low)
            lane = lax.broadcasted_iota(jnp.int32, (8, 128), 1)
            row = lax.broadcasted_iota(jnp.int32, (8, 128), 0)
            z[STEP : STEP + 8, :] = jnp.where((row == 0) & (lane < 64), edge[0:8, :128], got[64:72, :128])

    def send_chunk(c):
        def send(i, carry):
            t, where = target(i)
            pltpu.make_async_remote_copy(
                src_ref=x.at[c, t], dst_ref=o.at[c, me], send_sem=send_sem.at[c], recv_sem=recv_sem.at[c],
                device_id=where, device_id_type=MESH,
            ).start()
            return carry

        lax.fori_loop(1, 128, send, 0)
        o[c, me] = x[c, me]

    ready(6, 7, 8)
    for c in range(CHUNKS):
        for h in (0, 1):
            for jj in range((8 * h + PAIRS * c) // 2, (8 * h + PAIRS * (c + 1)) // 2):
                second_stage(jj)
        for block in range(128):
            q2, h = block // 2, block % 2
            start = STEP * 2 * (8 * h + PAIRS * c) + q2
            x[c, slot_of(block)] = z[pl.ds(start, LINES, stride=STEP), :]
        if c == 0:
            pl.semaphore_wait(barrier, 129)
            bins_part(0)
        if c == CHUNKS // 2:
            bins_part(1)
        send_chunk(c)

    first_block = (r == 0) & (m == 0)
    line = lax.broadcasted_iota(jnp.int32, (32, 128), 0)
    lane = lax.broadcasted_iota(jnp.int32, (32, 128), 1)
    p = lane + 128 * line
    signed = jnp.where(p >= SIDE // 2, p - SIDE, p)
    back = jnp.where(p == SIDE // 2, signed, -signed)
    half = lax.broadcasted_iota(jnp.int32, (64, 128), 1) // 64
    block = jnp.where(lower, 4 * r + m, 4 * (63 - r) + 2 + m)
    acc[...] = jnp.zeros_like(acc)

    ready(*range(9, 16))

    def spectrum(parts):
        high, low = split(jnp.concatenate([jnp.concatenate(part, 0) for part in parts], 1))
        mid = dot(tah[...], jnp.concatenate([high, low], 0)) + dot(tal[...], high)
        turned = []
        for k in (0, 1):
            re, im = mid[:64, 128 * k : 128 * k + 128], mid[64:, 128 * k : 128 * k + 128]
            re, im = jnp.concatenate([re, re], 0), jnp.concatenate([im, im], 0)
            turned.append(
                jnp.concatenate([re * cwc[...] - im * cws[...], re * cws[...] + im * cwc[...]], 1)
            )
        high, low = split(jnp.concatenate(turned, 0))
        last = dot_nt(tbh[...], high) + dot_nt(tbh[...], low) + dot_nt(tbl[...], high)
        return [
            (last[64 * c : 64 * c + 32, :128], last[64 * c + 32 : 64 * c + 64, :128],
             last[64 * c : 64 * c + 32, 128:], last[64 * c + 32 : 64 * c + 64, 128:])
            for c in (0, 1)
        ]

    def power_of(fields, freq_x, freq_y):
        radius = jnp.maximum(freq_x * freq_x + freq_y * freq_y, 1.0)
        cos_twice = (freq_x * freq_x - freq_y * freq_y) / radius
        sin_twice = 2.0 * freq_x * freq_y / radius
        q_re, q_im, u_re, u_im = fields
        e_re = cos_twice * q_re + sin_twice * u_re
        e_im = cos_twice * q_im + sin_twice * u_im
        b_re = cos_twice * u_re - sin_twice * q_re
        b_im = cos_twice * u_im - sin_twice * q_im
        scale = 1.0 / (SIDE * SIDE)
        terms = (e_re * e_re + e_im * e_im, b_re * b_re + b_im * b_im, e_re * b_re + e_im * b_im)
        return jnp.concatenate([(term * scale).astype(BF) for term in terms], 0)

    def reversed_lines(values):
        turned = dot(values, flip[...])
        parts = [turned[32 * k : 32 * k + 32] for k in range(3)]
        return jnp.concatenate([jnp.where(lane == 0, pltpu.roll(part, 31, 0), part) for part in parts], 0)

    want = lax.broadcasted_iota(jnp.int32, (32, 128), 0).astype(F32).astype(BF)
    wants = (want[:16], want[16:])
    one, none = jnp.ones((16, 128), BF), jnp.zeros((16, 128), BF)

    def add_up(items):
        total = acc[:, 0:32]
        for start in range(0, len(items), UNROLL):
            left, right = [], []
            for kind, c, row, hi, lo in items[start : start + UNROLL]:
                hot, cold = spread(hi(row)), spread(lo(row))
                vals = [spread(powers[kind, c, 32 * k + row : 32 * k + row + 1, :]) for k in range(3)]
                left.append(
                    jnp.concatenate([jnp.where(hot == w, val, none) for val in vals for w in wants], 0)
                )
                right.append(jnp.concatenate([jnp.where(cold == w, one, none) for w in wants], 0))
            total = total + dot_nt(jnp.concatenate(left, 1), jnp.concatenate(right, 1))
        acc[:, 0:32] = total

    def lines_of(ref, index, flipped):
        def get(row):
            at = 31 - row if flipped else row
            return ref[pl.ds(ref.shape[0] // 32 * at + index, 1), :]

        return get

    def pair_of(c, j):
        return [
            [o[c, pl.ds(64 * k, 64), pl.ds(2 * j + ri, 1), :].reshape(64, 128) for ri in (0, 1)] for k in (0, 1)
        ]

    def run_pair(c, j):
        fields = spectrum(pair_of(c, j))
        freq_y = signed.astype(F32)
        items = []
        for k in (0, 1):
            column = 2 * (PAIRS * c + j) + k
            freq_x = (16 * block + column).astype(F32)
            powers[0, k] = power_of(fields[k], freq_x, freq_y).astype(F32)
            powers[1, k] = reversed_lines(power_of(fields[k], -freq_x, back.astype(F32)))
            for row in range(32):
                items.append((0, k, row, lines_of(ahead_hi, column, False), lines_of(ahead_lo, column, False)))
        for k in (0, 1):
            column = 2 * (PAIRS * c + j) + k
            for row in range(32):
                items.append(
                    (1, k, row, lines_of(mirror_hi, 16 - column, True), lines_of(mirror_lo, 16 - column, True))
                )
        add_up(items)

    for c in range(CHUNKS):
        pltpu.make_async_copy(x.at[c, pl.ds(0, 127)], o.at[c, pl.ds(0, 127)], recv_sem.at[c]).wait()
        if c == 0:
            bins_ready(0)

            @pl.when(first_block)
            def _():
                parts = []
                for re, im in pair_of(0, 0):
                    parts.append([jnp.where(half == 0, re, pltpu.roll(im, 64, 1)), jnp.zeros((64, 128), F32)])
                fields = spectrum(parts)
                powers[0, 0] = power_of(fields[0], jnp.zeros((32, 128), F32), signed.astype(F32)).astype(F32)
                last = power_of(fields[1], jnp.full((32, 128), -(SIDE // 2) * 1.0, F32), back.astype(F32))
                powers[0, 1] = reversed_lines(last)
                items = [(0, 0, row, lines_of(ahead_hi, 0, False), lines_of(ahead_lo, 0, False)) for row in range(32)]
                items += [
                    (0, 1, row, lines_of(mirror_hi, 16, True), lines_of(mirror_lo, 16, True)) for row in range(32)
                ]
                add_up(items)
                ahead_hi[pl.ds(0, 32, stride=16), :] = jnp.full((32, 128), -1.0, F32)
                mirror_hi[pl.ds(16, 32, stride=24), :] = jnp.full((32, 128), -1.0, F32)

        if c == CHUNKS // 2:
            bins_ready(1)

        def body(j, carry):
            run_pair(c, j)
            return carry

        lax.fori_loop(0, PAIRS, body, 0)

    for c in range(CHUNKS):
        pltpu.make_async_copy(x.at[c, pl.ds(0, 127)], o.at[c, pl.ds(0, 127)], send_sem.at[c]).wait()

    wide = lax.broadcasted_iota(jnp.int32, (24, 128), 1) // 32
    part = jnp.zeros((24, 128), F32)
    for u in range(4):
        piece = acc[pl.ds(u, 24, stride=4), :]
        part = jnp.where(wide == u, piece if u == 0 else pltpu.roll(piece, 32 * u, 1), part)
    stage[0] = part
    peers = [[], [], []]
    for i in range(1, 8):
        peers[0].append({"rows": high_row * 8 + lax.rem(low_row + i, 8), "sky": s, "pair": m})
        peers[1].append({"rows": lax.rem(high_row + i, 8) * 8 + low_row, "sky": s, "pair": m})
    for i in range(1, 4):
        other = lax.rem(rep + i, 4)
        peers[2].append({"rows": r, "sky": other // 2, "pair": lax.rem(other, 2)})

    def phase(k, seen, here):
        count = len(peers[k])
        for where in peers[k]:
            pltpu.make_async_remote_copy(
                src_ref=stage.at[k], dst_ref=seen.at[here], send_sem=sum_send.at[k],
                recv_sem=sum_recv.at[k], device_id=where, device_id_type=MESH,
            ).start()
        seen[here] = stage[k]
        some = seen.at[pl.ds(0, count)]
        pltpu.make_async_copy(some, some, sum_send.at[k]).wait()
        pltpu.make_async_copy(some, some, sum_recv.at[k]).wait()

    phase(0, seen_a, low_row)
    stage[1] = jnp.sum(seen_a[...], axis=0)
    phase(1, seen_b, high_row)
    stage[2] = jnp.sum(seen_b[...], axis=0)
    phase(2, seen_c, rep)
    auto = NBINS / (SIDE * SIDE)
    for sky in (0, 1):
        whole = seen_c[2 * sky] + seen_c[2 * sky + 1]
        for k in range(3):
            for i in range(8):
                line_of = whole[8 * k + i : 8 * k + i + 1, :] * (auto if k < 2 else math.sqrt(auto))
                out[k, sky : sky + 1, 128 * i : 128 * i + 128] = line_of


def on_device(maps, mask, bins):
    tables = row_tables() + column_tables()
    loaded = (maps[0], mask) + tables
    here = pl.BlockSpec(memory_space=VMEM)
    there = pl.BlockSpec(memory_space=pltpu.HBM)
    dma = pltpu.SemaphoreType.DMA
    sums = pl.pallas_call(
        kernel,
        out_shape=jax.ShapeDtypeStruct((3, 2, NBINS), F32),
        in_specs=[there] * (3 + len(tables)),
        out_specs=here,
        scratch_shapes=[VMEM(one.shape, one.dtype) for one in loaded]
        + [
            VMEM((32, 64, 256), BF),
            VMEM((32, 64, 256), BF),
            VMEM((32 * STEP, 128), F32),
            VMEM((CHUNKS, 128, LINES, 128), F32),
            VMEM((CHUNKS, 128, LINES, 128), F32),
            VMEM((16, SIDE), jnp.int32),
            VMEM((24, SIDE), jnp.int32),
            VMEM((16 * 32, 128), F32),
            VMEM((16 * 32, 128), F32),
            VMEM((24 * 32, 128), F32),
            VMEM((24 * 32, 128), F32),
            VMEM((2, 2, 96, 128), F32),
            VMEM((96, 128), F32),
            VMEM((3, 24, 128), F32),
            VMEM((8, 24, 128), F32),
            VMEM((8, 24, 128), F32),
            VMEM((4, 24, 128), F32),
            dma((CHUNKS,)),
            dma((CHUNKS,)),
            dma((3,)),
            dma((3,)),
            dma((2,)),
            dma((3,)),
            dma((3,)),
            dma((16,)),
        ],
        compiler_params=pltpu.CompilerParams(
            collective_id=0, has_side_effects=True, vmem_limit_bytes=67043328
        ),
        name="sky_spectra",
    )(*loaded, bins.T)
    return jnp.transpose(sums, (1, 0, 2))


def solution(mesh):
    parted = Mesh(mesh.devices.reshape(mesh.shape["rows"], 2, 2), ("rows", "sky", "pair"))
    placed = (P(("sky", "pair"), "rows", None), P("rows", None), P(None, "rows"))
    return jax.shard_map(on_device, mesh=parted, in_specs=placed, out_specs=P(), check_vma=False)
```

```python
import functools
import math

import jax
import jax.numpy as jnp
import numpy as np
from jax import lax
from jax.experimental import pallas as pl
from jax.experimental.pallas import tpu as pltpu
from jax.sharding import Mesh
from jax.sharding import PartitionSpec as P

NBINS = 1024
SIDE = 4096
MESH = pl.DeviceIdType.MESH
BF = jnp.bfloat16
F32 = jnp.float32
VMEM = pltpu.VMEM
STEP = 72
CHUNKS = 4
BIN_AT = (1, 2)
LIMIT = 32 << 20
PAIRS = 8 // CHUNKS
LINES = 2 * PAIRS
UNROLL = 64


def halves(table):
    high = np.asarray(table, np.float32).astype(BF)
    low = (np.asarray(table, np.float64) - high.astype(np.float64)).astype(np.float32).astype(BF)
    return high, low


def angle(first, second, period):
    return 2.0 * np.pi * ((np.asarray(first)[:, None] * np.asarray(second)[None, :]) % period) / period


def row_tables():
    first = angle(np.arange(32), np.arange(32), 32)
    stage = np.concatenate([np.cos(first), -np.sin(first)], 0)
    first_high, first_low = halves(np.kron(stage, np.eye(8)))
    turn = angle(np.arange(32), np.arange(128), 4096)
    turn_cos = np.repeat(np.cos(turn), 8, 0).astype(np.float32)
    turn_sin = np.repeat(-np.sin(turn), 8, 0).astype(np.float32)
    last = angle(np.arange(64), np.arange(128), 128)
    cos, sin = np.cos(last), np.sin(last)
    last_high, last_low = halves(np.block([[cos, sin], [-sin, cos]]))
    alternate = np.zeros((16, 256), np.float32)
    alternate[0, :128] = 1.0 - 2.0 * (np.arange(128) % 2)
    return first_high, first_low, turn_cos, turn_sin, last_high, last_low, alternate.astype(BF)


def column_tables():
    first = angle(np.arange(64), np.arange(64), 64)
    cos, sin = np.cos(first), np.sin(first)
    high, low = halves(np.block([[cos, sin], [-sin, cos]]))
    doubled = np.concatenate([high, high], 1)
    turn = angle(np.arange(128), np.arange(64), 4096)
    turn_cos = np.tile(np.cos(turn), (1, 2)).astype(np.float32)
    turn_sin = np.tile(-np.sin(turn), (1, 2)).astype(np.float32)
    last = angle(np.arange(32), np.arange(64), 32)
    cos, sin = np.cos(last), np.sin(last)
    none = np.zeros_like(cos)
    last_high, last_low = halves(
        np.block(
            [
                [cos, none, sin, none],
                [-sin, none, cos, none],
                [none, cos, none, sin],
                [none, -sin, none, cos],
            ]
        )
    )
    flip = np.zeros((128, 128), np.float32)
    flip[(128 - np.arange(128)) % 128, np.arange(128)] = 1.0
    return doubled, low, turn_cos, turn_sin, last_high, last_low, flip.astype(BF)


def split(values):
    high = values.astype(BF)
    return high, (values - high.astype(F32)).astype(BF)


def dot(left, right):
    return jnp.dot(left, right, preferred_element_type=F32)


def dot_nt(left, right):
    return lax.dot_general(left, right, (((1,), (1,)), ((), ())), preferred_element_type=F32)


def slot_of(block):
    group, part = block // 4, block % 4
    return (part % 2) * 64 + (group if part < 2 else 63 - group)


def spread(line):
    tile = jnp.broadcast_to(line, (8, 128))
    return jnp.concatenate([tile, tile], 0).astype(BF)


def kernel(*refs):
    (maps, mask, bins, narrow, wide, out), refs = refs[:6], refs[6:]
    held, rest = refs[:16], refs[16:]
    arrived = rest[-1]
    sources = [maps, mask]
    at = [0, 0]
    for one in held[2:]:
        if one.dtype == BF:
            sources.append(narrow.at[pl.ds(at[0], one.shape[0]), pl.ds(0, one.shape[1])])
            at[0] += one.shape[0]
        else:
            sources.append(wide.at[pl.ds(at[1], one.shape[0])])
            at[1] += one.shape[0]
    for i in range(16):
        pltpu.make_async_copy(sources[i], held[i], arrived.at[i]).start()

    def ready(*places):
        for i in places:
            pltpu.make_async_copy(sources[i], held[i], arrived.at[i]).wait()

    work(ready, bins, out, *held, *rest[:-1])


def work(
    ready, bins, out,
    maps, mask, t1h, t1l, twc, tws, t2h, t2l, alt, tah, tal, cwc, cws, tbh, tbl, flip,
    yh, yl, z, x, o, ahead, mirror, ahead_hi, ahead_lo, mirror_hi, mirror_lo, powers, acc,
    stage, seen_a, seen_b, seen_c, send_sem, recv_sem, bin_send, bin_recv, bin_here, sum_send, sum_recv,
):
    r, s, m = lax.axis_index("rows"), lax.axis_index("sky"), lax.axis_index("pair")
    me = m * 64 + r
    lower = r < 32
    low_row, high_row = lax.rem(r, 8), r // 8
    rep = 2 * s + m

    def over_sky(action):
        def other_map(i, carry):
            action(lax.rem(r + i, 64), 1 - m)
            return carry

        def same_map(i, carry):
            action(lax.rem(r + i, 64), m)
            return carry

        lax.fori_loop(0, 64, other_map, 0)
        lax.fori_loop(1, 64, same_map, 0)

    barrier = pltpu.get_barrier_semaphore()

    def greet(row, pair):
        where = {"rows": row, "sky": s, "pair": pair}
        pl.semaphore_signal(barrier, inc=1, device_id=where, device_id_type=MESH)

    over_sky(greet)
    for pair in (0, 1):
        pl.semaphore_signal(
            barrier, inc=1, device_id={"rows": r, "sky": 1 - s, "pair": pair}, device_id_type=MESH
        )

    @pl.when(lower)
    def _():
        pltpu.make_async_copy(bins.at[pl.ds(16 * m, 16)], ahead, bin_here.at[0]).start()

    @pl.when(jnp.logical_not(lower))
    def _():
        pltpu.make_async_copy(bins.at[pl.ds(16 - 16 * m, 16)], mirror.at[pl.ds(0, 16)], bin_here.at[0]).start()
        pltpu.make_async_copy(bins.at[pl.ds(32 - 16 * m, 1)], mirror.at[pl.ds(16, 1)], bin_here.at[1]).start()

    partner = {"rows": 63 - r, "sky": s, "pair": m}

    def bins_part(k):
        def ship(source, count, place, where, sem=k):
            pltpu.make_async_remote_copy(
                src_ref=bins.at[pl.ds(source, count)], dst_ref=place, send_sem=bin_send.at[sem],
                recv_sem=bin_recv.at[sem], device_id=where, device_id_type=MESH,
            ).start()

        @pl.when(lower)
        def _():
            ship(32 + 16 * m + 8 * k, 8, ahead.at[pl.ds(8 * k, 8)], partner)

        @pl.when(jnp.logical_not(lower))
        def _():
            ship(56 - 16 * m - 8 * k, 8, mirror.at[pl.ds(8 - 8 * k, 8)], partner)
            if k == 0:
                beside = lax.rem(64 - r, 32) * (1 - m) + (63 - r) * m
                ship(48 * m, 1, mirror.at[pl.ds(16, 1)], {"rows": beside, "sky": s, "pair": m}, 2)

    def bins_ready(k):
        def wait(count, sem):
            pltpu.make_async_copy(bins.at[pl.ds(0, count)], mirror.at[pl.ds(0, count)], sem).wait()

        @pl.when(lower)
        def _():
            wait(8, bin_recv.at[k])
            wait(8, bin_send.at[k])
            if k == 0:
                wait(16, bin_here.at[0])
                wait(1, bin_recv.at[2])

        @pl.when(jnp.logical_not(lower))
        def _():
            wait(8, bin_recv.at[k])
            wait(8, bin_send.at[k])
            if k == 0:
                wait(16, bin_here.at[0])
                wait(1, bin_here.at[1])
                wait(1, bin_send.at[2])

        rows = [(ahead, ahead_hi, ahead_lo, 8 * k, 8), (mirror, mirror_hi, mirror_lo, 8 - 8 * k, 8)]
        if k == 0:
            rows.append((mirror, mirror_hi, mirror_lo, 16, 1))
        for src, hi, lo, start, count in rows:
            size = src.shape[0]
            for i in range(32):
                part = src[start : start + count, 128 * i : 128 * i + 128]
                hi[size * i + start : size * i + start + count, :] = (part >> 5).astype(F32)
                lo[size * i + start : size * i + start + count, :] = (part & 31).astype(F32)

    ready(0, 1, 2, 3, 4, 5)
    turn_cos, turn_sin = twc[...].reshape(32, 8, 128), tws[...].reshape(32, 8, 128)
    for g in range(0, 8, 2):
        pair = []
        for k in (g, g + 1):
            rows = maps[8 * k : 8 * k + 8, :] * mask[8 * k : 8 * k + 8, :].astype(F32)
            pair.append(jnp.concatenate([rows[:, 128 * a : 128 * a + 128] for a in range(32)], 0))
        high, low = split(jnp.concatenate(pair, 1))
        got = dot(t1h[...], high) + dot(t1h[...], low) + dot(t1l[...], high)
        real = got[:256].reshape(32, 8, 256)
        imag = got[256:].reshape(32, 8, 256)
        for k in (0, 1):
            re, im = real[:, :, 128 * k : 128 * k + 128], imag[:, :, 128 * k : 128 * k + 128]
            pair[k] = (re * turn_cos - im * turn_sin, re * turn_sin + im * turn_cos)
        for part in (0, 1):
            high, low = split(jnp.concatenate([pair[0][part], pair[1][part]], 1))
            yh[:, 8 * g : 8 * g + 16, 128 * part : 128 * part + 128] = high
            yl[:, 8 * g : 8 * g + 16, 128 * part : 128 * part + 128] = low

    def second_stage(jj):
        high = yh[4 * jj : 4 * jj + 4].reshape(256, 256)
        low = yl[4 * jj : 4 * jj + 4].reshape(256, 256)
        got = dot_nt(t2h[...], high) + dot_nt(t2h[...], low) + dot_nt(t2l[...], high)
        for k in (0, 1):
            for ri in (0, 1):
                start = STEP * (2 * (2 * jj + k) + ri)
                z[start : start + 64, :] = got[64 * ri : 64 * ri + 64, 128 * k : 128 * k + 128]
        if jj == 0:
            edge = dot_nt(alt[...], high) + dot_nt(alt[...], low)
            lane = lax.broadcasted_iota(jnp.int32, (8, 128), 1)
            row = lax.broadcasted_iota(jnp.int32, (8, 128), 0)
            z[STEP : STEP + 8, :] = jnp.where((row == 0) & (lane < 64), edge[0:8, :128], got[64:72, :128])

    def send_chunk(c):
        def send(row, pair):
            pltpu.make_async_remote_copy(
                src_ref=x.at[c, 64 * pair + row], dst_ref=o.at[c, me], send_sem=send_sem.at[c],
                recv_sem=recv_sem.at[c], device_id={"rows": row, "sky": s, "pair": pair}, device_id_type=MESH,
            ).start()

        over_sky(send)
        o[c, me] = x[c, me]

    ready(6, 7, 8)
    for c in range(CHUNKS):
        for h in (0, 1):
            for jj in range((8 * h + PAIRS * c) // 2, (8 * h + PAIRS * (c + 1)) // 2):
                second_stage(jj)
        for block in range(128):
            q2, h = block // 2, block % 2
            start = STEP * 2 * (8 * h + PAIRS * c) + q2
            x[c, slot_of(block)] = z[pl.ds(start, LINES, stride=STEP), :]
        if c == 0:
            pl.semaphore_wait(barrier, 129)
        for k in (0, 1):
            if BIN_AT[k] == c:
                bins_part(k)
        send_chunk(c)

    first_block = (r == 0) & (m == 0)
    line = lax.broadcasted_iota(jnp.int32, (32, 128), 0)
    lane = lax.broadcasted_iota(jnp.int32, (32, 128), 1)
    p = lane + 128 * line
    signed = jnp.where(p >= SIDE // 2, p - SIDE, p)
    back = jnp.where(p == SIDE // 2, signed, -signed)
    half = lax.broadcasted_iota(jnp.int32, (64, 128), 1) // 64
    block = jnp.where(lower, 4 * r + m, 4 * (63 - r) + 2 + m)
    acc[...] = jnp.zeros_like(acc)

    ready(*range(9, 16))

    def spectrum(parts):
        high, low = split(jnp.concatenate([jnp.concatenate(part, 0) for part in parts], 1))
        mid = dot(tah[...], jnp.concatenate([high, low], 0)) + dot(tal[...], high)
        turned = []
        for k in (0, 1):
            re, im = mid[:64, 128 * k : 128 * k + 128], mid[64:, 128 * k : 128 * k + 128]
            re, im = jnp.concatenate([re, re], 0), jnp.concatenate([im, im], 0)
            turned.append(
                jnp.concatenate([re * cwc[...] - im * cws[...], re * cws[...] + im * cwc[...]], 1)
            )
        high, low = split(jnp.concatenate(turned, 0))
        last = dot_nt(tbh[...], high) + dot_nt(tbh[...], low) + dot_nt(tbl[...], high)
        return [
            (last[64 * c : 64 * c + 32, :128], last[64 * c + 32 : 64 * c + 64, :128],
             last[64 * c : 64 * c + 32, 128:], last[64 * c + 32 : 64 * c + 64, 128:])
            for c in (0, 1)
        ]

    def power_of(fields, freq_x, freq_y):
        radius = jnp.maximum(freq_x * freq_x + freq_y * freq_y, 1.0)
        cos_twice = (freq_x * freq_x - freq_y * freq_y) / radius
        sin_twice = 2.0 * freq_x * freq_y / radius
        q_re, q_im, u_re, u_im = fields
        e_re = cos_twice * q_re + sin_twice * u_re
        e_im = cos_twice * q_im + sin_twice * u_im
        b_re = cos_twice * u_re - sin_twice * q_re
        b_im = cos_twice * u_im - sin_twice * q_im
        scale = 1.0 / (SIDE * SIDE)
        terms = (e_re * e_re + e_im * e_im, b_re * b_re + b_im * b_im, e_re * b_re + e_im * b_im)
        return jnp.concatenate([(term * scale).astype(BF) for term in terms], 0)

    def reversed_lines(values):
        turned = dot(values, flip[...])
        parts = [turned[32 * k : 32 * k + 32] for k in range(3)]
        return jnp.concatenate([jnp.where(lane == 0, pltpu.roll(part, 31, 0), part) for part in parts], 0)

    want = lax.broadcasted_iota(jnp.int32, (32, 128), 0).astype(F32).astype(BF)
    wants = (want[:16], want[16:])
    one, none = jnp.ones((16, 128), BF), jnp.zeros((16, 128), BF)

    def add_up(items):
        total = acc[:, 0:32]
        for start in range(0, len(items), UNROLL):
            left, right = [], []
            for kind, c, row, hi, lo in items[start : start + UNROLL]:
                hot, cold = spread(hi(row)), spread(lo(row))
                vals = [spread(powers[kind, c, 32 * k + row : 32 * k + row + 1, :]) for k in range(3)]
                left.append(
                    jnp.concatenate([jnp.where(hot == w, val, none) for val in vals for w in wants], 0)
                )
                right.append(jnp.concatenate([jnp.where(cold == w, one, none) for w in wants], 0))
            total = total + dot_nt(jnp.concatenate(left, 1), jnp.concatenate(right, 1))
        acc[:, 0:32] = total

    def lines_of(ref, index, flipped):
        def get(row):
            at = 31 - row if flipped else row
            return ref[pl.ds(ref.shape[0] // 32 * at + index, 1), :]

        return get

    def pair_of(c, j):
        return [
            [o[c, pl.ds(64 * k, 64), pl.ds(2 * j + ri, 1), :].reshape(64, 128) for ri in (0, 1)] for k in (0, 1)
        ]

    def run_pair(c, j):
        fields = spectrum(pair_of(c, j))
        freq_y = signed.astype(F32)
        items = []
        for k in (0, 1):
            column = 2 * (PAIRS * c + j) + k
            freq_x = (16 * block + column).astype(F32)
            powers[0, k] = power_of(fields[k], freq_x, freq_y).astype(F32)
            powers[1, k] = reversed_lines(power_of(fields[k], -freq_x, back.astype(F32)))
            for row in range(32):
                items.append((0, k, row, lines_of(ahead_hi, column, False), lines_of(ahead_lo, column, False)))
        for k in (0, 1):
            column = 2 * (PAIRS * c + j) + k
            for row in range(32):
                items.append(
                    (1, k, row, lines_of(mirror_hi, 16 - column, True), lines_of(mirror_lo, 16 - column, True))
                )
        add_up(items)

    for c in range(CHUNKS):
        pltpu.make_async_copy(x.at[c, pl.ds(0, 127)], o.at[c, pl.ds(0, 127)], recv_sem.at[c]).wait()
        if c == 0:
            bins_ready(0)

            @pl.when(first_block)
            def _():
                parts = []
                for re, im in pair_of(0, 0):
                    parts.append([jnp.where(half == 0, re, pltpu.roll(im, 64, 1)), jnp.zeros((64, 128), F32)])
                fields = spectrum(parts)
                powers[0, 0] = power_of(fields[0], jnp.zeros((32, 128), F32), signed.astype(F32)).astype(F32)
                last = power_of(fields[1], jnp.full((32, 128), -(SIDE // 2) * 1.0, F32), back.astype(F32))
                powers[0, 1] = reversed_lines(last)
                items = [(0, 0, row, lines_of(ahead_hi, 0, False), lines_of(ahead_lo, 0, False)) for row in range(32)]
                items += [
                    (0, 1, row, lines_of(mirror_hi, 16, True), lines_of(mirror_lo, 16, True)) for row in range(32)
                ]
                add_up(items)
                ahead_hi[pl.ds(0, 32, stride=16), :] = jnp.full((32, 128), -1.0, F32)
                mirror_hi[pl.ds(16, 32, stride=24), :] = jnp.full((32, 128), -1.0, F32)

        if c == CHUNKS // 2:
            bins_ready(1)

        def body(j, carry):
            run_pair(c, j)
            return carry

        lax.fori_loop(0, PAIRS, body, 0)

    for c in range(CHUNKS):
        pltpu.make_async_copy(x.at[c, pl.ds(0, 127)], o.at[c, pl.ds(0, 127)], send_sem.at[c]).wait()

    wide = lax.broadcasted_iota(jnp.int32, (24, 128), 1) // 32
    part = jnp.zeros((24, 128), F32)
    for u in range(4):
        piece = acc[pl.ds(u, 24, stride=4), :]
        part = jnp.where(wide == u, piece if u == 0 else pltpu.roll(piece, 32 * u, 1), part)
    stage[0] = part
    peers = [[], [], []]
    for i in range(1, 8):
        peers[0].append({"rows": high_row * 8 + lax.rem(low_row + i, 8), "sky": s, "pair": m})
        peers[1].append({"rows": lax.rem(high_row + i, 8) * 8 + low_row, "sky": s, "pair": m})
    for i in range(1, 4):
        other = lax.rem(rep + i, 4)
        peers[2].append({"rows": r, "sky": other // 2, "pair": lax.rem(other, 2)})

    def phase(k, seen, here):
        count = len(peers[k])
        for where in peers[k]:
            pltpu.make_async_remote_copy(
                src_ref=stage.at[k], dst_ref=seen.at[here], send_sem=sum_send.at[k],
                recv_sem=sum_recv.at[k], device_id=where, device_id_type=MESH,
            ).start()
        seen[here] = stage[k]
        some = seen.at[pl.ds(0, count)]
        pltpu.make_async_copy(some, some, sum_send.at[k]).wait()
        pltpu.make_async_copy(some, some, sum_recv.at[k]).wait()

    phase(0, seen_a, low_row)
    stage[1] = jnp.sum(seen_a[...], axis=0)
    phase(1, seen_b, high_row)
    stage[2] = jnp.sum(seen_b[...], axis=0)
    phase(2, seen_c, rep)
    auto = NBINS / (SIDE * SIDE)
    for sky in (0, 1):
        whole = seen_c[2 * sky] + seen_c[2 * sky + 1]
        for k in range(3):
            for i in range(8):
                line_of = whole[8 * k + i : 8 * k + i + 1, :] * (auto if k < 2 else math.sqrt(auto))
                out[k, sky : sky + 1, 128 * i : 128 * i + 128] = line_of


def on_device(maps, mask, bins):
    tables = row_tables() + column_tables()
    loaded = (maps[0], mask) + tables
    narrow = [np.pad(one, ((0, 0), (0, 256 - one.shape[1]))) for one in tables if one.dtype == BF]
    wide = [one for one in tables if one.dtype != BF]
    here = pl.BlockSpec(memory_space=VMEM)
    there = pl.BlockSpec(memory_space=pltpu.HBM)
    dma = pltpu.SemaphoreType.DMA
    sums = pl.pallas_call(
        kernel,
        out_shape=jax.ShapeDtypeStruct((3, 2, NBINS), F32),
        in_specs=[there] * 5,
        out_specs=here,
        scratch_shapes=[VMEM(one.shape, one.dtype) for one in loaded]
        + [
            VMEM((32, 64, 256), BF),
            VMEM((32, 64, 256), BF),
            VMEM((32 * STEP, 128), F32),
            VMEM((CHUNKS, 128, LINES, 128), F32),
            VMEM((CHUNKS, 128, LINES, 128), F32),
            VMEM((16, SIDE), jnp.int32),
            VMEM((24, SIDE), jnp.int32),
            VMEM((16 * 32, 128), F32),
            VMEM((16 * 32, 128), F32),
            VMEM((24 * 32, 128), F32),
            VMEM((24 * 32, 128), F32),
            VMEM((2, 2, 96, 128), F32),
            VMEM((96, 128), F32),
            VMEM((3, 24, 128), F32),
            VMEM((8, 24, 128), F32),
            VMEM((8, 24, 128), F32),
            VMEM((4, 24, 128), F32),
            dma((CHUNKS,)),
            dma((CHUNKS,)),
            dma((3,)),
            dma((3,)),
            dma((2,)),
            dma((3,)),
            dma((3,)),
            dma((16,)),
        ],
        compiler_params=pltpu.CompilerParams(
            collective_id=0, has_side_effects=True, vmem_limit_bytes=LIMIT
        ),
        name="sky_spectra",
    )(*[pltpu.with_memory_space_constraint(one, pltpu.HBM) for one in (maps[0], mask, bins.T, jnp.asarray(np.concatenate(narrow, 0)), jnp.asarray(np.concatenate(wide, 0)))])
    return jnp.transpose(sums, (1, 0, 2))


def solution(mesh):
    parted = Mesh(mesh.devices.reshape(mesh.shape["rows"], 2, 2), ("rows", "sky", "pair"))
    placed = (P(("sky", "pair"), "rows", None), P("rows", None), P(None, "rows"))
    return jax.shard_map(on_device, mesh=parted, in_specs=placed, out_specs=P(), check_vma=False)
```
